32 devices in a mesh: groups: 2 (over x), lon: 8 (over z, y), lat: 2 (over core).
Axes of the slice: x: 2, y: 2, z: 4, core: 2. Of those that a mesh axis runs over, the one named last changes fastest.
Arguments:
- fields: bfloat16 [24, 1024, 128], P(('groups', 'lat'), 'lon'), parts along dimension 0, may hold values from -6 to 6
- norm_gain: float32 [128], replicated, may hold values from 0.5 to 1.5
- w_qkv: bfloat16 [128, 384], replicated, may hold values from -5.303301 to 5.303301
- w_out: bfloat16 [128, 128], replicated, may hold values from -0.5 to 0.5
Outputs:
- updated: bfloat16 [24, 1024, 128], P(('groups', 'lat'), 'lon'), parts along dimension 0
The draws below stay inside these ranges and needn't reach their ends.
There are 2 independent parts, one for each index of `groups`. The reference program is written for one: setup_inputs(seed, part) draws one part's arguments, and reference() takes and returns one part's arrays. A program takes and returns all parts, laid end to end along the dimension named above; an argument that names none is the same for every part. Nothing has to cross between parts.
All inputs are finite; a program needn't handle non-finite values.
Results may differ from the reference program's by a relative error of at most 0.005.
The reference program's roundings to bfloat16 on the way (of `normed`, `weights` and `attended`) count: a program that leaves them out, or rounds other values in their place, can miss the bound.
Values may be sent and summed in bfloat16 or wider, within the bound.
A program may use at most 128 MiB of HBM per device.

```python
import math
import jax
import jax.numpy as jnp
from jax import lax

HEADS = 8
HEAD_DIM = 16
C = 128
NLON = 1024
NLAT = 12


def draw_w_qkv(key, part):
    base = jnp.clip(jax.random.normal(key, (C, 3 * C), jnp.float32), -6.0, 6.0) * (2.0 / math.sqrt(C))
    return base.astype(jnp.bfloat16)


def block_scale(stream_key, shape, shards, low, high):
    def one(position, shards_of):
        steps = jax.random.uniform(jax.random.fold_in(jax.random.fold_in(stream_key, 6), position), (shards_of,), jnp.float32, low / len(shards), high / len(shards))
        return jnp.repeat(jnp.exp(steps), shape[position] // shards_of).reshape((-1,) + (1,) * (len(shape) - position - 1))

    loudness = one(*shards[0])
    for cut in shards[1:]:
        loudness = loudness * one(*cut)
    return loudness


def bell_draw(rng, dims, scale, bound, split=(), kind=jnp.bfloat16):
    values = scale * jax.random.normal(rng, dims, jnp.float32)
    if split:
        values = values * block_scale(rng, dims, split, -0.22, 0.18)
    return jnp.clip(values, -bound, bound).astype(kind)


def setup_inputs(seed: int = 0, part: int = 0) -> dict:
    key_list = jax.random.split(jax.random.key(seed), 5)
    part_keys = jax.random.split(jax.random.fold_in(key_list[4], part), 5)
    fields = bell_draw(part_keys[0], (NLAT, NLON, C), 1.0, 6.0, ((0, 2), (1, 8)))
    norm_gain = jnp.clip(1.0 + 0.1 * jax.random.normal(key_list[1], (C,), jnp.float32), 0.5, 1.5)
    w_qkv = draw_w_qkv(jax.random.fold_in(key_list[4], 71), part)
    w_out = bell_draw(key_list[3], (C, C), C ** -0.5, 0.5)
    return {"fields": fields, "norm_gain": norm_gain, "w_qkv": w_qkv, "w_out": w_out}


def reference(fields, norm_gain, w_qkv, w_out):
    width = HEADS * HEAD_DIM
    inputs = fields.astype(jnp.float32)
    center = lax.optimization_barrier(jnp.mean(inputs, axis=-1, keepdims=True))
    spread = lax.optimization_barrier(jnp.mean((inputs - center) ** 2, axis=-1, keepdims=True))
    normed = ((inputs - center) * lax.rsqrt(spread + 1e-05) * norm_gain).astype(jnp.bfloat16)
    projected = jnp.dot(normed.reshape(-1, width), w_qkv, preferred_element_type=jnp.float32)
    projected = projected.reshape(NLAT, NLON, 3 * width)
    queries = (projected[..., :width] * (1.0 / math.sqrt(HEAD_DIM))).astype(jnp.bfloat16)
    keys = projected[..., width:2 * width].astype(jnp.bfloat16)
    values = projected[..., 2 * width:].astype(jnp.bfloat16)
    block = math.gcd(NLON, 512)

    def one_row(operands):
        row_queries, row_keys, row_values = operands
        key_heads = row_keys.reshape(NLON, HEADS, HEAD_DIM).astype(jnp.float32)
        value_heads = row_values.reshape(NLON, HEADS, HEAD_DIM).astype(jnp.float32)
        query_blocks = row_queries.reshape(NLON // block, block, HEADS, HEAD_DIM)

        def one_block(query_block):
            scores = jnp.einsum('qhd,khd->hqk', query_block.astype(jnp.float32), key_heads)
            highest = lax.optimization_barrier(jnp.max(scores, axis=-1, keepdims=True))
            expd = jnp.exp(scores - highest)
            totals = lax.optimization_barrier(jnp.sum(expd, axis=-1))
            weights = expd.astype(jnp.bfloat16).astype(jnp.float32)
            mixed = jnp.einsum('hqk,khd->qhd', weights, value_heads)
            mixed = mixed / jnp.transpose(totals)[:, :, None]
            return mixed.reshape(block, width).astype(jnp.bfloat16)
        return lax.map(one_block, query_blocks).reshape(NLON, width)
    attended = lax.map(one_row, (queries, keys, values))
    output = jnp.dot(attended.reshape(-1, width), w_out, preferred_element_type=jnp.float32)
    return (inputs + output.reshape(NLAT, NLON, width)).astype(jnp.bfloat16)
```

```python
import functools
import math

import jax
import jax.numpy as jnp
from jax import lax
from jax.experimental import pallas as pl
from jax.experimental.pallas import tpu as pltpu
from jax.sharding import PartitionSpec as P

HEADS = 8
LOG2E = math.log2(math.e)
MESH = pl.DeviceIdType.MESH


def dot(a, b, contract):
    return lax.dot_general(a, b, ((contract[:1], contract[1:]), ((), ())), preferred_element_type=jnp.float32)


def kernel(n, per, slots, fields_ref, gain_ref, wqkv_ref, wout_ref, out_ref,
           normed, whole, w_t, scores_a, scores_b, mixed, returned,
           send1, recv1, send2, recv2):
    me = lax.axis_index("lon")
    rows, cells, width = fields_ref.shape
    head_width = width // HEADS
    total = n * cells
    block = math.gcd(total, 256)
    chunk = math.gcd(total, 256)

    barrier = pltpu.get_barrier_semaphore()
    for k in range(1, n):
        pl.semaphore_signal(barrier, inc=1, device_id={"lon": lax.rem(me + k, n)}, device_id_type=MESH)

    gain = gain_ref[...]
    for r in range(rows):
        inputs = fields_ref[r].astype(jnp.float32)
        center = jnp.mean(inputs, axis=-1, keepdims=True)
        spread = jnp.mean((inputs - center) ** 2, axis=-1, keepdims=True)
        normed[r] = ((inputs - center) * lax.rsqrt(spread + 1e-05) * gain).astype(jnp.bfloat16)

    def first_row(d):
        return (d * per) // HEADS

    def last_row(d):
        return (d * per + per - 1) // HEADS

    pl.semaphore_wait(barrier, n - 1)

    def forward(j, k):
        d = lax.rem(me + k, n)
        return d, pltpu.make_async_remote_copy(
            src_ref=normed.at[first_row(d) + j],
            dst_ref=whole.at[j, me],
            send_sem=send1.at[j, k],
            recv_sem=recv1.at[j, me],
            device_id={"lon": d},
            device_id_type=MESH,
        )

    for j in range(slots):
        for k in range(1, n):
            d, copy = forward(j, k)

            @pl.when(first_row(d) + j <= last_row(d))
            def _():
                copy.start()

    for j in range(slots):
        @pl.when(first_row(me) + j <= last_row(me))
        def _():
            whole[j, me] = normed[first_row(me) + j]

    w_t[...] = wqkv_ref[...].astype(jnp.float32).T.astype(jnp.bfloat16)

    def back(t, k):
        d = lax.rem(me + k, n)
        return pltpu.make_async_remote_copy(
            src_ref=mixed.at[t, d],
            dst_ref=returned.at[me * per + t],
            send_sem=send2.at[t, k],
            recv_sem=recv2.at[me * per + t],
            device_id={"lon": d},
            device_id_type=MESH,
        )

    def one_item(t, carry):
        item = me * per + t
        head = lax.rem(item, HEADS)
        slot = item // HEADS - first_row(me)

        @pl.when((t == 0) | (head == 0))
        def _():
            for k in range(1, n):
                src = lax.rem(me + k, n)
                pltpu.make_async_remote_copy(
                    src_ref=normed.at[0],
                    dst_ref=whole.at[slot, src],
                    send_sem=send1.at[0, 0],
                    recv_sem=recv1.at[slot, src],
                    device_id={"lon": src},
                    device_id_type=MESH,
                ).wait_recv()

        cell_rows = whole[slot].reshape(total, width)

        def weight(part):
            start = pl.multiple_of(part * width + head * head_width, head_width)
            return w_t[pl.ds(start, head_width), :]

        w_k = weight(1)
        q_t = (dot(weight(0), cell_rows, (1, 1)) * (1.0 / math.sqrt(head_width))).astype(jnp.bfloat16)
        q_t = q_t.astype(jnp.float32) * LOG2E
        q_hi = q_t.astype(jnp.bfloat16)
        q_lo = (q_t - q_hi.astype(jnp.float32)).astype(jnp.bfloat16)
        q_pair = jnp.concatenate([q_hi, q_lo], axis=0)
        keys = dot(cell_rows, jnp.concatenate([w_k, w_k], axis=0), (1, 1)).astype(jnp.bfloat16)
        v_t = dot(weight(2), cell_rows, (1, 1)).astype(jnp.bfloat16)

        buffers = (scores_a, scores_b)

        def first_pass(b):
            q_block = q_pair[:, b * block:(b + 1) * block]
            highest = None
            for c in range(total // chunk):
                s = dot(keys[c * chunk:(c + 1) * chunk], q_block, (1, 0))
                buffers[b % 2][pl.ds(c * chunk, chunk), :] = s
                part = jnp.max(s.reshape(chunk // 8, 8, block), axis=0)
                highest = part if highest is None else jnp.maximum(highest, part)
            return jnp.max(highest, axis=0, keepdims=True)

        def second_pass(b, highest):
            sums = jnp.zeros((8, block), jnp.float32)
            acc = jnp.zeros((head_width, block), jnp.float32)
            for c in range(total // chunk):
                p = jnp.exp2(buffers[b % 2][pl.ds(c * chunk, chunk), :] - highest)
                sums = sums + jnp.sum(p.reshape(chunk // 8, 8, block), axis=0)
                acc = acc + dot(v_t[:, c * chunk:(c + 1) * chunk], p.astype(jnp.bfloat16), (1, 0))
            return (acc / jnp.sum(sums, axis=0, keepdims=True)).astype(jnp.bfloat16)

        blocks = total // block
        highest = first_pass(0)
        for b in range(blocks):
            following = first_pass(b + 1) if b + 1 < blocks else None
            done = second_pass(b, highest)
            highest = following
            for s in range(block // cells):
                mixed[t, b * (block // cells) + s] = done[:, s * cells:(s + 1) * cells]

        returned[item] = mixed[t, me]
        for k in range(1, n):
            back(t, k).start()
        return carry

    lax.fori_loop(0, per, one_item, 0)

    def finish(t, carry):
        for k in range(1, n):
            src = lax.rem(me + k, n)
            pltpu.make_async_remote_copy(
                src_ref=mixed.at[0, 0],
                dst_ref=returned.at[src * per + t],
                send_sem=send2.at[t, k],
                recv_sem=recv2.at[src * per + t],
                device_id={"lon": src},
                device_id_type=MESH,
            ).wait_recv()
        return carry

    lax.fori_loop(0, per, finish, 0)

    for r in range(rows):
        att_t = returned[pl.ds(r * HEADS, HEADS)].reshape(width, cells)
        update = dot(att_t, wout_ref[...], (0, 0))
        out_ref[r] = (fields_ref[r].astype(jnp.float32) + update).astype(jnp.bfloat16)

    for j in range(slots):
        for k in range(1, n):
            d, copy = forward(j, k)

            @pl.when(first_row(d) + j <= last_row(d))
            def _():
                copy.wait_send()

    def sent(t, carry):
        for k in range(1, n):
            back(t, k).wait_send()
        return carry

    lax.fori_loop(0, per, sent, 0)


def solution(mesh):
    n = mesh.shape["lon"]

    def body(fields, norm_gain, w_qkv, w_out):
        rows, cells, width = fields.shape
        per = rows * HEADS // n
        slots = max((d * per + per - 1) // HEADS - (d * per) // HEADS + 1 for d in range(n))
        total = n * cells
        block = math.gcd(total, 256)
        return pl.pallas_call(
            functools.partial(kernel, n, per, slots),
            out_shape=jax.ShapeDtypeStruct(fields.shape, fields.dtype),
            in_specs=[pl.BlockSpec(memory_space=pltpu.VMEM)] * 4,
            out_specs=pl.BlockSpec(memory_space=pltpu.VMEM),
            scratch_shapes=[
                pltpu.VMEM((rows, cells, width), jnp.bfloat16),
                pltpu.VMEM((slots, n, cells, width), jnp.bfloat16),
                pltpu.VMEM((3 * width, width), jnp.bfloat16),
                pltpu.VMEM((total, block), jnp.float32),
                pltpu.VMEM((total, block), jnp.float32),
                pltpu.VMEM((per, n, width // HEADS, cells), jnp.bfloat16),
                pltpu.VMEM((rows * HEADS, width // HEADS, cells), jnp.bfloat16),
                pltpu.SemaphoreType.DMA((slots, n)),
                pltpu.SemaphoreType.DMA((slots, n)),
                pltpu.SemaphoreType.DMA((per, n)),
                pltpu.SemaphoreType.DMA((rows * HEADS,)),
            ],
            compiler_params=pltpu.CompilerParams(collective_id=0, has_side_effects=True),
        )(fields, norm_gain.reshape(1, width), w_qkv, w_out)

    return jax.shard_map(
        body,
        mesh=mesh,
        in_specs=(P(("groups", "lat"), "lon", None), P(), P(), P()),
        out_specs=P(("groups", "lat"), "lon", None),
        check_vma=False,
    )
```

```python
import functools
import math

import jax
import jax.numpy as jnp
from jax import lax
from jax.experimental import pallas as pl
from jax.experimental.pallas import tpu as pltpu
from jax.sharding import PartitionSpec as P

HEADS = 8
LOG2E = math.log2(math.e)
MESH = pl.DeviceIdType.MESH


def dot(a, b, contract):
    return lax.dot_general(a, b, ((contract[:1], contract[1:]), ((), ())), preferred_element_type=jnp.float32)


def kernel(n, per, slots, fields_ref, gain_ref, wqkv_ref, wout_ref, out_ref,
           normed, whole, w_t, scores_a, scores_b, scores_c, q_s, k_s, v_s,
           mixed, returned,
           send1, recv1, send2, recv2):
    me = lax.axis_index("lon")
    rows, cells, width = fields_ref.shape
    head_width = width // HEADS
    total = n * cells
    block = math.gcd(total, 512)
    chunk = math.gcd(total, 256)

    def partner(k):
        if n & (n - 1):
            return lax.rem(me + n - k, n)
        mate = 0
        for bit in range(n.bit_length() - 1):
            own = lax.rem(me // (1 << bit), 2)
            mate = mate + ((1 - own) if (k >> bit) & 1 else own) * (1 << bit)
        return mate

    barrier = pltpu.get_barrier_semaphore()
    for k in range(1, n):
        pl.semaphore_signal(barrier, inc=1, device_id={"lon": lax.rem(me + k, n)}, device_id_type=MESH)

    gain = gain_ref[...]
    for r in range(rows):
        inputs = fields_ref[r].astype(jnp.float32)
        center = jnp.mean(inputs, axis=-1, keepdims=True)
        spread = jnp.mean((inputs - center) ** 2, axis=-1, keepdims=True)
        normed[r] = ((inputs - center) * lax.rsqrt(spread + 1e-05) * gain).astype(jnp.bfloat16)

    def first_row(d):
        return (d * per) // HEADS

    def last_row(d):
        return (d * per + per - 1) // HEADS

    pl.semaphore_wait(barrier, n - 1)

    def forward(j, k):
        d = partner(k)
        return d, pltpu.make_async_remote_copy(
            src_ref=normed.at[first_row(d) + j],
            dst_ref=whole.at[j, me],
            send_sem=send1.at[j, k],
            recv_sem=recv1.at[j, me],
            device_id={"lon": d},
            device_id_type=MESH,
        )

    for j in range(slots):
        for k in range(n - 1, 0, -1):
            d, copy = forward(j, k)

            @pl.when(first_row(d) + j <= last_row(d))
            def _():
                copy.start()

    for j in range(slots):
        @pl.when(first_row(me) + j <= last_row(me))
        def _():
            whole[j, me] = normed[first_row(me) + j]

    w_t[...] = wqkv_ref[...].astype(jnp.float32).T.astype(jnp.bfloat16)

    def back(t, k):
        d = partner(k)
        return pltpu.make_async_remote_copy(
            src_ref=mixed.at[t, d],
            dst_ref=returned.at[me * per + t],
            send_sem=send2.at[t, k],
            recv_sem=recv2.at[me * per + t],
            device_id={"lon": d},
            device_id_type=MESH,
        )

    def wait_slot(slot):
        for k in range(1, n):
            src = lax.rem(me + k, n)
            pltpu.make_async_remote_copy(
                src_ref=normed.at[0],
                dst_ref=whole.at[slot, src],
                send_sem=send1.at[0, 0],
                recv_sem=recv1.at[slot, src],
                device_id={"lon": src},
                device_id_type=MESH,
            ).wait_recv()

    def project(item):
        head = lax.rem(item, HEADS)
        cell_rows = whole[item // HEADS - first_row(me)].reshape(total, width)

        def weight(part):
            start = pl.multiple_of(part * width + head * head_width, head_width)
            return w_t[pl.ds(start, head_width), :]

        w_k = weight(1)
        q_t = (dot(weight(0), cell_rows, (1, 1)) * (1.0 / math.sqrt(head_width))).astype(jnp.bfloat16)
        q_t = q_t.astype(jnp.float32) * LOG2E
        q_hi = q_t.astype(jnp.bfloat16)
        q_lo = (q_t - q_hi.astype(jnp.float32)).astype(jnp.bfloat16)
        q_s[...] = jnp.concatenate([q_hi, q_lo], axis=0)
        k_s[...] = dot(cell_rows, jnp.concatenate([w_k, w_k], axis=0), (1, 1)).astype(jnp.bfloat16)
        v_s[...] = dot(weight(2), cell_rows, (1, 1)).astype(jnp.bfloat16)

    def buffer(b):
        return scores_c if b == 0 else (scores_a, scores_b)[b % 2]

    def first_pass(b, queries, keys):
        q_block = queries[:, b * block:(b + 1) * block]
        highest = None
        for c in range(total // chunk):
            s = dot(keys[c * chunk:(c + 1) * chunk], q_block, (1, 0))
            buffer(b)[pl.ds(c * chunk, chunk), :] = s
            part = jnp.max(s.reshape(chunk // 8, 8, block), axis=0)
            highest = part if highest is None else jnp.maximum(highest, part)
        return jnp.max(highest, axis=0, keepdims=True)

    def second_pass(b, highest, v_t):
        sums = jnp.zeros((8, block), jnp.float32)
        acc = jnp.zeros((head_width, block), jnp.float32)
        for c in range(total // chunk):
            p = jnp.exp2(buffer(b)[pl.ds(c * chunk, chunk), :] - highest)
            sums = sums + jnp.sum(p.reshape(chunk // 8, 8, block), axis=0)
            acc = acc + dot(v_t[:, c * chunk:(c + 1) * chunk], p.astype(jnp.bfloat16), (1, 0))
        return (acc / jnp.sum(sums, axis=0, keepdims=True)).astype(jnp.bfloat16)

    def one_item(t, highest):
        item = me * per + t
        after = jnp.minimum(item + 1, me * per + per - 1)

        @pl.when((t + 1 < per) & (lax.rem(item + 1, HEADS) == 0))
        def _():
            wait_slot(after // HEADS - first_row(me))

        queries, keys, v_t = q_s[...], k_s[...], v_s[...]
        project(after)
        blocks = total // block
        for b in range(blocks):
            if b + 1 < blocks:
                following = first_pass(b + 1, queries, keys)
            done = second_pass(b, highest, v_t)
            if b + 1 == blocks:
                following = first_pass(0, q_s[...], k_s[...])
            highest = following
            for s in range(block // cells):
                mixed[t, b * (block // cells) + s] = done[:, s * cells:(s + 1) * cells]

        returned[item] = mixed[t, me]
        for k in range(n - 1, 0, -1):
            back(t, k).start()
        return highest

    wait_slot(0)
    project(me * per)
    lax.fori_loop(0, per, one_item, first_pass(0, q_s[...], k_s[...]))

    def finish(t, carry):
        for k in range(1, n):
            src = lax.rem(me + k, n)
            pltpu.make_async_remote_copy(
                src_ref=mixed.at[0, 0],
                dst_ref=returned.at[src * per + t],
                send_sem=send2.at[t, k],
                recv_sem=recv2.at[src * per + t],
                device_id={"lon": src},
                device_id_type=MESH,
            ).wait_recv()
        return carry

    lax.fori_loop(0, per, finish, 0)

    for r in range(rows):
        att_t = returned[pl.ds(r * HEADS, HEADS)].reshape(width, cells)
        update = dot(att_t, wout_ref[...], (0, 0))
        out_ref[r] = (fields_ref[r].astype(jnp.float32) + update).astype(jnp.bfloat16)

    for j in range(slots):
        for k in range(1, n):
            d, copy = forward(j, k)

            @pl.when(first_row(d) + j <= last_row(d))
            def _():
                copy.wait_send()

    def sent(t, carry):
        for k in range(1, n):
            back(t, k).wait_send()
        return carry

    lax.fori_loop(0, per, sent, 0)


def solution(mesh):
    n = mesh.shape["lon"]

    def body(fields, norm_gain, w_qkv, w_out):
        rows, cells, width = fields.shape
        per = rows * HEADS // n
        slots = max((d * per + per - 1) // HEADS - (d * per) // HEADS + 1 for d in range(n))
        total = n * cells
        block = math.gcd(total, 512)
        return pl.pallas_call(
            functools.partial(kernel, n, per, slots),
            out_shape=jax.ShapeDtypeStruct(fields.shape, fields.dtype),
            in_specs=[pl.BlockSpec(memory_space=pltpu.VMEM)] * 4,
            out_specs=pl.BlockSpec(memory_space=pltpu.VMEM),
            scratch_shapes=[
                pltpu.VMEM((rows, cells, width), jnp.bfloat16),
                pltpu.VMEM((slots, n, cells, width), jnp.bfloat16),
                pltpu.VMEM((3 * width, width), jnp.bfloat16),
                pltpu.VMEM((total, block), jnp.float32),
                pltpu.VMEM((total, block), jnp.float32),
                pltpu.VMEM((total, block), jnp.float32),
                pltpu.VMEM((2 * width // HEADS, total), jnp.bfloat16),
                pltpu.VMEM((total, 2 * width // HEADS), jnp.bfloat16),
                pltpu.VMEM((width // HEADS, total), jnp.bfloat16),
                pltpu.VMEM((per, n, width // HEADS, cells), jnp.bfloat16),
                pltpu.VMEM((rows * HEADS, width // HEADS, cells), jnp.bfloat16),
                pltpu.SemaphoreType.DMA((slots, n)),
                pltpu.SemaphoreType.DMA((slots, n)),
                pltpu.SemaphoreType.DMA((per, n)),
                pltpu.SemaphoreType.DMA((rows * HEADS,)),
            ],
            compiler_params=pltpu.CompilerParams(collective_id=0, has_side_effects=True),
        )(fields, norm_gain.reshape(1, width), w_qkv, w_out)

    return jax.shard_map(
        body,
        mesh=mesh,
        in_specs=(P(("groups", "lat"), "lon", None), P(), P(), P()),
        out_specs=P(("groups", "lat"), "lon", None),
        check_vma=False,
    )
```

```python
import functools
import math

import jax
import jax.numpy as jnp
from jax import lax
from jax.experimental import pallas as pl
from jax.experimental.pallas import tpu as pltpu
from jax.sharding import PartitionSpec as P

HEADS = 8
LOG2E = math.log2(math.e)
MESH = pl.DeviceIdType.MESH


def dot(a, b, contract):
    return lax.dot_general(a, b, ((contract[:1], contract[1:]), ((), ())), preferred_element_type=jnp.float32)


def kernel(n, per, slots, fields_ref, gain_ref, wqkv_ref, returned,
           normed, whole, w_t, scores_a, scores_b, scores_c, q_s, k_s, v_s,
           mixed,
           send1, recv1, send2, recv2):
    me = lax.axis_index("lon")
    rows, cells, width = fields_ref.shape
    head_width = width // HEADS
    total = n * cells
    block = math.gcd(total, 512)
    chunk = math.gcd(total, 256)

    def partner(k):
        if n & (n - 1):
            return lax.rem(me + n - k, n)
        mate = 0
        for bit in range(n.bit_length() - 1):
            own = lax.rem(me // (1 << bit), 2)
            mate = mate + ((1 - own) if (k >> bit) & 1 else own) * (1 << bit)
        return mate

    barrier = pltpu.get_barrier_semaphore()
    for k in range(1, n):
        pl.semaphore_signal(barrier, inc=1, device_id={"lon": lax.rem(me + k, n)}, device_id_type=MESH)

    gain = gain_ref[...]
    for r in range(rows):
        inputs = fields_ref[r].astype(jnp.float32)
        center = jnp.mean(inputs, axis=-1, keepdims=True)
        spread = jnp.mean((inputs - center) ** 2, axis=-1, keepdims=True)
        normed[r] = ((inputs - center) * lax.rsqrt(spread + 1e-05) * gain).astype(jnp.bfloat16)

    def first_row(d):
        return (d * per) // HEADS

    def last_row(d):
        return (d * per + per - 1) // HEADS

    pl.semaphore_wait(barrier, n - 1)

    def forward(j, k):
        d = partner(k)
        return d, pltpu.make_async_remote_copy(
            src_ref=normed.at[first_row(d) + j],
            dst_ref=whole.at[j, me],
            send_sem=send1.at[j, k],
            recv_sem=recv1.at[j, me],
            device_id={"lon": d},
            device_id_type=MESH,
        )

    for j in range(slots):
        for k in range(n - 1, 0, -1):
            d, copy = forward(j, k)

            @pl.when(first_row(d) + j <= last_row(d))
            def _():
                copy.start()

    for j in range(slots):
        @pl.when(first_row(me) + j <= last_row(me))
        def _():
            whole[j, me] = normed[first_row(me) + j]

    w_t[...] = wqkv_ref[...].astype(jnp.float32).T.astype(jnp.bfloat16)

    def back(t, k):
        d = partner(k)
        return pltpu.make_async_remote_copy(
            src_ref=mixed.at[t, d],
            dst_ref=returned.at[me * per + t],
            send_sem=send2.at[t, k],
            recv_sem=recv2.at[me * per + t],
            device_id={"lon": d},
            device_id_type=MESH,
        )

    def wait_slot(slot):
        for k in range(1, n):
            src = lax.rem(me + k, n)
            pltpu.make_async_remote_copy(
                src_ref=normed.at[0],
                dst_ref=whole.at[slot, src],
                send_sem=send1.at[0, 0],
                recv_sem=recv1.at[slot, src],
                device_id={"lon": src},
                device_id_type=MESH,
            ).wait_recv()

    def project(item):
        head = lax.rem(item, HEADS)
        cell_rows = whole[item // HEADS - first_row(me)].reshape(total, width)

        def weight(part):
            start = pl.multiple_of(part * width + head * head_width, head_width)
            return w_t[pl.ds(start, head_width), :]

        w_k = weight(1)
        q_t = (dot(weight(0), cell_rows, (1, 1)) * (1.0 / math.sqrt(head_width))).astype(jnp.bfloat16)
        q_t = q_t.astype(jnp.float32) * LOG2E
        q_hi = q_t.astype(jnp.bfloat16)
        q_lo = (q_t - q_hi.astype(jnp.float32)).astype(jnp.bfloat16)
        q_s[...] = jnp.concatenate([q_hi, q_lo], axis=0)
        k_s[...] = dot(cell_rows, jnp.concatenate([w_k, w_k], axis=0), (1, 1)).astype(jnp.bfloat16)
        v_s[...] = dot(weight(2), cell_rows, (1, 1)).astype(jnp.bfloat16)

    def buffer(b):
        return scores_c if b == 0 else (scores_a, scores_b)[b % 2]

    def first_pass(b, queries, keys):
        q_block = queries[:, b * block:(b + 1) * block]
        highest = None
        for c in range(total // chunk):
            s = dot(keys[c * chunk:(c + 1) * chunk], q_block, (1, 0))
            buffer(b)[pl.ds(c * chunk, chunk), :] = s
            part = jnp.max(s.reshape(chunk // 8, 8, block), axis=0)
            highest = part if highest is None else jnp.maximum(highest, part)
        return jnp.max(highest, axis=0, keepdims=True)

    def second_pass(b, highest, v_t):
        sums = jnp.zeros((8, block), jnp.float32)
        acc = jnp.zeros((head_width, block), jnp.float32)
        for c in range(total // chunk):
            p = jnp.exp2(buffer(b)[pl.ds(c * chunk, chunk), :] - highest)
            sums = sums + jnp.sum(p.reshape(chunk // 8, 8, block), axis=0)
            acc = acc + dot(v_t[:, c * chunk:(c + 1) * chunk], p.astype(jnp.bfloat16), (1, 0))
        return (acc / jnp.sum(sums, axis=0, keepdims=True)).astype(jnp.bfloat16)

    def one_item(t, highest):
        item = me * per + t
        after = jnp.minimum(item + 1, me * per + per - 1)

        @pl.when((t + 1 < per) & (lax.rem(item + 1, HEADS) == 0))
        def _():
            wait_slot(after // HEADS - first_row(me))

        queries, keys, v_t = q_s[...], k_s[...], v_s[...]
        project(after)
        blocks = total // block
        for b in range(blocks):
            if b + 1 < blocks:
                following = first_pass(b + 1, queries, keys)
            done = second_pass(b, highest, v_t)
            if b + 1 == blocks:
                following = first_pass(0, q_s[...], k_s[...])
            highest = following
            for s in range(block // cells):
                mixed[t, b * (block // cells) + s] = done[:, s * cells:(s + 1) * cells]

        returned[item] = mixed[t, me]
        for k in range(n - 1, 0, -1):
            back(t, k).start()
        return highest

    wait_slot(0)
    project(me * per)
    lax.fori_loop(0, per, one_item, first_pass(0, q_s[...], k_s[...]))

    def finish(t, carry):
        for k in range(1, n):
            src = lax.rem(me + k, n)
            pltpu.make_async_remote_copy(
                src_ref=mixed.at[0, 0],
                dst_ref=returned.at[src * per + t],
                send_sem=send2.at[t, k],
                recv_sem=recv2.at[src * per + t],
                device_id={"lon": src},
                device_id_type=MESH,
            ).wait_recv()
        return carry

    lax.fori_loop(0, per, finish, 0)

    for j in range(slots):
        for k in range(1, n):
            d, copy = forward(j, k)

            @pl.when(first_row(d) + j <= last_row(d))
            def _():
                copy.wait_send()

    def sent(t, carry):
        for k in range(1, n):
            back(t, k).wait_send()
        return carry

    lax.fori_loop(0, per, sent, 0)


def solution(mesh):
    n = mesh.shape["lon"]

    def body(fields, norm_gain, w_qkv, w_out):
        rows, cells, width = fields.shape
        per = rows * HEADS // n
        slots = max((d * per + per - 1) // HEADS - (d * per) // HEADS + 1 for d in range(n))
        total = n * cells
        block = math.gcd(total, 512)
        att_t = pl.pallas_call(
            functools.partial(kernel, n, per, slots),
            out_shape=jax.ShapeDtypeStruct((rows * HEADS, width // HEADS, cells), fields.dtype),
            in_specs=[pl.BlockSpec(memory_space=pltpu.VMEM)] * 3,
            out_specs=pl.BlockSpec(memory_space=pltpu.VMEM),
            scratch_shapes=[
                pltpu.VMEM((rows, cells, width), jnp.bfloat16),
                pltpu.VMEM((slots, n, cells, width), jnp.bfloat16),
                pltpu.VMEM((3 * width, width), jnp.bfloat16),
                pltpu.VMEM((total, block), jnp.float32),
                pltpu.VMEM((total, block), jnp.float32),
                pltpu.VMEM((total, block), jnp.float32),
                pltpu.VMEM((2 * width // HEADS, total), jnp.bfloat16),
                pltpu.VMEM((total, 2 * width // HEADS), jnp.bfloat16),
                pltpu.VMEM((width // HEADS, total), jnp.bfloat16),
                pltpu.VMEM((per, n, width // HEADS, cells), jnp.bfloat16),
                pltpu.SemaphoreType.DMA((slots, n)),
                pltpu.SemaphoreType.DMA((slots, n)),
                pltpu.SemaphoreType.DMA((per, n)),
                pltpu.SemaphoreType.DMA((rows * HEADS,)),
            ],
            compiler_params=pltpu.CompilerParams(collective_id=0, has_side_effects=True),
        )(fields, norm_gain.reshape(1, width), w_qkv)
        update = jnp.einsum('rcl,cd->rld', att_t.reshape(rows, width, cells), w_out, preferred_element_type=jnp.float32)
        return (fields.astype(jnp.float32) + update).astype(jnp.bfloat16)

    return jax.shard_map(
        body,
        mesh=mesh,
        in_specs=(P(("groups", "lat"), "lon", None), P(), P(), P()),
        out_specs=P(("groups", "lat"), "lon", None),
        check_vma=False,
    )
```
